32 devices in a mesh: rep: 2 (over x), tp: 8 (over z, y), sub: 2 (over core).
Axes of the slice: x: 2, y: 2, z: 4, core: 2. Of those that a mesh axis runs over, the one named last changes fastest.
Arguments:
- attention: bfloat16 [1024, 8192], P('rep', ('tp', 'sub')), parts along dimension 0, may hold values from -6 to 6
- out_weight: bfloat16 [8192, 8192], P(('tp', 'sub')), may hold values from -0.09375 to 0.09375
- residual: bfloat16 [1024, 8192], P('rep', ('tp', 'sub')), parts along dimension 0, may hold values from -6 to 6
- norm_gain: bfloat16 [8192], P(('tp', 'sub')), may hold values from 0.25 to 1.75
Outputs:
- quantized: bfloat16 [1024, 8192], P('rep'), parts along dimension 0
- scales: bfloat16 [1024, 64], P('rep'), parts along dimension 0
- new_residual: bfloat16 [1024, 8192], P('rep', ('tp', 'sub')), parts along dimension 0
The draws below stay inside these ranges and needn't reach their ends.
There are 2 independent parts, one for each index of `rep`. The reference program is written for one: setup_inputs(seed, part) draws one part's arguments, and reference() takes and returns one part's arrays. A program takes and returns all parts, laid end to end along the dimension named above; an argument that names none is the same for every part. Nothing has to cross between parts.
All inputs are finite; a program needn't handle non-finite values.
Results may differ from the reference program's by a relative error of at most 0.0048.
Values may be sent and summed in bfloat16 or wider, within the bound.
A program may use at most 128 MiB of HBM per device.

```python
import jax
import jax.numpy as jnp
from jax import lax

D = 8192
BLOCK = 128
ROWS = 512


def with_spikes(drawn, own_key, source, target, shards_of, factor):
    owner, partner = [(jnp.arange(drawn.shape[position]) // (drawn.shape[position] // shards_of)).reshape([-1 if axis == position else 1 for axis in range(drawn.ndim)]) for position in (source, target)]
    chosen = jax.random.permutation(own_key, shards_of)[partner]
    strong = (owner == chosen) | (owner == (partner + shards_of // 2) % shards_of)
    return jnp.where(strong, factor * drawn, drawn)


def block_scale(stream_key, shape, split, low, top_value):
    def one(dim, parts):
        steps = jax.random.uniform(jax.random.fold_in(jax.random.fold_in(stream_key, 6), dim), (parts,), jnp.float32, low / len(split), top_value / len(split))
        return jnp.repeat(jnp.exp(steps), shape[dim] // parts).reshape((-1,) + (1,) * (len(shape) - dim - 1))

    loudness = one(*split[0])
    for cut in split[1:]:
        loudness = loudness * one(*cut)
    return loudness


def gaussian(own_key, shape, width, most, pieces=(), dtype=jnp.bfloat16):
    array = width * jax.random.normal(own_key, shape, jnp.float32)
    if pieces:
        array = array * block_scale(own_key, shape, pieces, -0.22, 0.18)
    return jnp.clip(array, -most, most).astype(dtype)


def heavy_noise(own_key, shape, scale, limit, split, heavy, kind=jnp.bfloat16):
    entries = scale * jax.random.normal(own_key, shape, jnp.float32)
    if split:
        entries = entries * block_scale(own_key, shape, split, -0.22, 0.18)
    return jnp.clip(with_spikes(entries, jax.random.fold_in(own_key, 3), *heavy), -limit, limit).astype(kind)


def setup_inputs(seed: int = 0, part: int = 0) -> dict:
    key_of = jax.random.split(jax.random.key(seed), 5)
    own_keys = jax.random.split(jax.random.fold_in(key_of[4], part), 5)
    return {
        "attention": gaussian(own_keys[0], (ROWS, D), 1.0, 6.0, ((1, 16),)),
        "out_weight": heavy_noise(key_of[1], (D, D), D ** -0.5, 0.09375, ((0, 16),), (0, 1, 16, 2.0)),
        "residual": gaussian(own_keys[2], (ROWS, D), 1.0, 6.0, ((1, 16),)),
        "norm_gain": jnp.clip(1.0 + 0.15 * jax.random.normal(key_of[3], (D,), jnp.float32), 0.25, 1.75).astype(jnp.bfloat16),
    }


epsilon = 0.1
floor_scale = 0.5

def reference(attention, out_weight, residual, norm_gain):
    projected = jnp.dot(attention, out_weight, preferred_element_type=jnp.float32)
    hidden = residual.astype(jnp.float32) + projected
    new_residual = hidden.astype(jnp.bfloat16)
    mean_square = lax.optimization_barrier(jnp.mean(hidden * hidden, axis=1, keepdims=True))
    normed = hidden * lax.rsqrt(mean_square + epsilon) * norm_gain.astype(jnp.float32)
    blocks = normed.reshape(hidden.shape[0], hidden.shape[1] // BLOCK, BLOCK)
    largest = lax.optimization_barrier(jnp.max(jnp.abs(blocks), axis=2))
    scales = jnp.maximum(largest, floor_scale).astype(jnp.bfloat16)
    quantized = (blocks / scales.astype(jnp.float32)[:, :, None]).reshape(hidden.shape).astype(jnp.bfloat16)
    return (quantized, scales, new_residual)
```

```python
import functools

import jax
import jax.numpy as jnp
from jax import lax
from jax.experimental import pallas as pl
from jax.experimental.pallas import tpu as pltpu
from jax.sharding import PartitionSpec as P

BLOCK = 128
LANES = 128
MESH = pl.DeviceIdType.MESH

epsilon = 0.1
floor_scale = 0.5


def loop(n, body):
    if n <= 8:
        for i in range(n):
            body(i)
    else:
        lax.fori_loop(0, n, lambda i, c: (body(i), c)[1], 0)


def kernel(
    Y, Z, U, C, R, width_all,
    att, weight, res, gain,
    quant, scales, new_res,
    att_p, w_own, w_par, ysend, ybuf, zsend, zbuf, hid, stat, sct, scfull,
    l_sem, xs_sem, xr_sem, as_sem, ar_sem, ys_sem, yr_sem, zs_sem, zr_sem,
    ss_sem, sr_sem, cs_sem, cr_sem, qzs, qzr, qys, qyr, qus, qur,
):
    T = Y * Z
    n = T * U
    w = res.shape[1]
    nb = w // BLOCK
    tp = lax.axis_index("tp")
    s = lax.axis_index("sub")
    z = tp // Y
    y = lax.rem(tp, Y)
    me = tp * U + s
    other = (U - 1) - s
    f32 = jnp.float32

    def cols(t, sub):
        return pl.ds(pl.multiple_of((t * U + sub) * w, w), w)

    def rows(c):
        return pl.ds(c * R, R)

    def rc(src, dst, ss, rs, t, sub):
        return pltpu.make_async_remote_copy(
            src_ref=src, dst_ref=dst, send_sem=ss, recv_sem=rs,
            device_id={"tp": t, "sub": sub}, device_id_type=MESH,
        )

    yp = (Y - 1) - y
    zt = lambda zz: zz * Y + y
    zo = lambda k: lax.rem(z + k, Z)
    order = lambda i: (i % Z) * Y + (yp if i < Z else y) if Y > 1 else i

    def wload(t):
        return pltpu.make_async_copy(weight.at[:, cols(t, s)], w_own.at[t], l_sem.at[t])

    def wpush(t):
        return rc(weight.at[:, cols(t, other)], w_par.at[t], xs_sem.at[t], xr_sem.at[t], tp, other)

    apush = rc(att, att_p, as_sem, ar_sem, tp, other)

    loop(T, lambda i: wload(order(i)).start())
    barrier = pltpu.get_barrier_semaphore()

    def greet(k):
        p = lax.rem(me + k + 1, n)
        pl.semaphore_signal(
            barrier, inc=1, device_id={"tp": p // U, "sub": lax.rem(p, U)}, device_id_type=MESH
        )

    loop(n - 1, greet)
    pl.semaphore_wait(barrier, n - 1)
    apush.start()
    loop(T, lambda i: wpush(order(i)).start())
    apush.wait()

    def w_wait(t):
        wload(t).wait()
        wpush(t).wait_recv()

    def product(c, t):
        a = jnp.dot(att[rows(c), :], w_own[t], preferred_element_type=f32)
        return a + jnp.dot(att_p[rows(c), :], w_par[t], preferred_element_type=f32)

    def ycopy(c):
        return rc(ysend.at[c], ybuf.at[c], ys_sem.at[c], yr_sem.at[c], z * Y + yp, s)

    def zcopy(c, zz):
        return rc(zsend.at[c, zz], zbuf.at[c, z], zs_sem.at[c, zz], zr_sem.at[c, z], zt(zz), s)

    def zwait(c, zz):
        rc(zsend.at[c, zz], zbuf.at[c, zz], zs_sem.at[c, zz], zr_sem.at[c, zz], zt(zz), s).wait_recv()

    if Y > 1:
        for c in range(C):
            def one(zz, c=c):
                t = zz * Y + yp
                if c == 0:
                    w_wait(t)
                ysend[c, zz] = product(c, t).astype(ysend.dtype)
            loop(Z, one)
            ycopy(c).start()

    def s4(c):
        if Y > 1:
            ycopy(c).wait_recv()

        def total(zz):
            t = zt(zz)
            if c == 0:
                w_wait(t)
            a = product(c, t)
            if Y > 1:
                a = a + ybuf[c, zz].astype(f32)
            return a

        def one(k):
            zz = zo(k + 1)
            zsend[c, zz] = total(zz).astype(zsend.dtype)
            zcopy(c, zz).start()

        loop(Z - 1, one)
        hid[c] = total(z) + res[rows(c), :].astype(f32)

    def peer(k):
        p = lax.rem(me + k + 1, n)
        return p, p // U, lax.rem(p, U)

    def scopy(c, p, t, u, slot):
        return rc(stat.at[c, me], stat.at[c, slot], ss_sem.at[c, p], sr_sem.at[c, slot], t, u)

    def ccopy(c, p, t, u, slot):
        return rc(sct.at[c, me], sct.at[c, slot], cs_sem.at[c, p], cr_sem.at[c, slot], t, u)

    def s5(c):
        def add(k):
            zz = zo(k + 1)
            zwait(c, zz)
            hid[c] = hid[c] + zbuf[c, zz].astype(f32)

        loop(Z - 1, add)
        h = hid[c]
        new_res[rows(c), :] = h.astype(new_res.dtype)
        sq = jnp.sum(h * h, axis=1, keepdims=True)
        stat[c, me] = jnp.broadcast_to(sq, (R, LANES)).T[0:1, :]

        def send(k):
            p, t, u = peer(k)
            scopy(c, p, t, u, me).start()

        loop(n - 1, send)

    def qz(c, zz):
        sl = quant.at[rows(c), cols(tp, s)]
        return rc(sl, sl, qzs.at[c, zz], qzr.at[c, z], zt(zz), s)

    def qz_wait(c, zz):
        sl = quant.at[rows(c), cols(zt(zz), s)]
        rc(sl, sl, qzs.at[c, zz], qzr.at[c, zz], zt(zz), s).wait_recv()

    def qy(c, zz, yy):
        sl = quant.at[rows(c), cols(zz * Y + yy, s)]
        return rc(sl, sl, qys.at[c, zz], qyr.at[c, zz], z * Y + yp, s)

    def qu(c, t, u):
        sl = quant.at[rows(c), cols(t, u)]
        return rc(sl, sl, qus.at[c, t], qur.at[c, t], tp, other)

    def s6(c):
        def w_stat(k):
            p, t, u = peer(k)
            scopy(c, p, t, u, p).wait_recv()

        loop(n - 1, w_stat)
        tot = jnp.sum(stat[c], axis=0)
        col = jnp.broadcast_to(tot, (LANES, R)).T
        inv = lax.rsqrt(col / width_all + epsilon)
        for j in range(nb):
            sl = slice(j * BLOCK, (j + 1) * BLOCK)
            nr = hid[c, :, sl] * inv * gain[:, sl].astype(f32)
            sc = jnp.maximum(jnp.max(jnp.abs(nr), axis=1, keepdims=True), floor_scale)
            sc = jnp.broadcast_to(sc.astype(jnp.bfloat16).astype(f32), (R, BLOCK))
            quant[rows(c), pl.ds(pl.multiple_of(me * w + j * BLOCK, BLOCK), BLOCK)] = (
                nr / sc
            ).astype(quant.dtype)
            sct[c, me, j : j + 1, :] = sc.T[0:1, :]
        loop(Z - 1, lambda k: qz(c, zo(k + 1)).start())
        if Y > 1:
            qy(c, z, y).start()

        def send(k):
            p, t, u = peer(k)
            ccopy(c, p, t, u, me).start()

        loop(n - 1, send)
        qu(c, tp, s).start()

    def s7(c):
        def one(k):
            zz = zo(k + 1)
            qz_wait(c, zz)
            if Y > 1:
                qy(c, zz, y).start()
            qu(c, zt(zz), s).start()

        loop(Z - 1, one)

    def s8(c):
        if Y > 1:
            def one(k):
                zz = zo(k)
                qy(c, zz, yp).wait_recv()
                qu(c, zz * Y + yp, s).start()

            loop(Z, one)

    def s9(c):
        def w_c(k):
            p, t, u = peer(k)
            ccopy(c, p, t, u, p).wait_recv()

        loop(n - 1, w_c)
        for d in range(n):
            scfull[d * nb : (d + 1) * nb, :] = sct[c, d]
        scales[rows(c), :] = scfull[...].T[:, : n * nb].astype(scales.dtype)
        loop(T, lambda t: qu(c, t, other).wait_recv())

    stages = (s4, s5, s6, s7, s8, s9)
    for i in range(C + len(stages) - 1):
        for j, stage in enumerate(stages):
            if 0 <= i - j < C:
                stage(i - j)

    loop(T, lambda t: wpush(t).wait_send())
    for c in range(C):
        if Y > 1:
            ycopy(c).wait_send()
            loop(Z, lambda zz, c=c: qy(c, zz, y).wait_send())

        def zdone(k, c=c):
            zcopy(c, zo(k + 1)).wait_send()
            qz(c, zo(k + 1)).wait_send()

        loop(Z - 1, zdone)

        def pdone(k, c=c):
            p, t, u = peer(k)
            scopy(c, p, t, u, me).wait_send()
            ccopy(c, p, t, u, me).wait_send()

        loop(n - 1, pdone)
        loop(T, lambda t, c=c: qu(c, t, s).wait_send())


def per_device(Y, Z, U, attention, out_weight, residual, norm_gain):
    M, K = attention.shape
    width_all = out_weight.shape[1]
    w = residual.shape[1]
    T = Y * Z
    n = T * U
    R = LANES
    C = M // R
    nb = w // BLOCK
    bf = jnp.bfloat16
    dma = pltpu.SemaphoreType.DMA
    vm = pl.BlockSpec(memory_space=pltpu.VMEM)
    return pl.pallas_call(
        functools.partial(kernel, Y, Z, U, C, R, width_all),
        out_shape=(
            jax.ShapeDtypeStruct((M, width_all), bf),
            jax.ShapeDtypeStruct((M, width_all // BLOCK), bf),
            jax.ShapeDtypeStruct((M, w), bf),
        ),
        in_specs=[vm, pl.BlockSpec(memory_space=pl.ANY), vm, vm],
        out_specs=(vm, vm, vm),
        scratch_shapes=[
            pltpu.VMEM((M, K), bf),
            pltpu.VMEM((T, K, w), bf),
            pltpu.VMEM((T, K, w), bf),
            pltpu.VMEM((C, Z, R, w), bf),
            pltpu.VMEM((C, Z, R, w), bf),
            pltpu.VMEM((C, Z, R, w), bf),
            pltpu.VMEM((C, Z, R, w), bf),
            pltpu.VMEM((C, R, w), jnp.float32),
            pltpu.VMEM((C, n, 1, R), jnp.float32),
            pltpu.VMEM((C, n, nb, R), jnp.float32),
            pltpu.VMEM((-(-n * nb // LANES) * LANES, R), jnp.float32),
            dma((T,)), dma((T,)), dma((T,)), dma, dma,
            dma((C,)), dma((C,)), dma((C, Z)), dma((C, Z)),
            dma((C, n)), dma((C, n)), dma((C, n)), dma((C, n)),
            dma((C, Z)), dma((C, Z)), dma((C, Z)), dma((C, Z)), dma((C, T)), dma((C, T)),
        ],
        compiler_params=pltpu.CompilerParams(
            collective_id=0, has_side_effects=True, vmem_limit_bytes=60 * 1024 * 1024
        ),
        cost_estimate=pl.CostEstimate(
            flops=2 * M * K * width_all, bytes_accessed=2 * K * width_all, transcendentals=0
        ),
    )(attention, out_weight, residual, norm_gain.reshape(1, w))


def inner_count(mesh):
    chips = [tuple(getattr(d, "coords", (0, 0, i))) for i, d in enumerate(mesh.devices[0, :, 0].flat)]
    count = sum(1 for c in chips if c[2] == chips[0][2])
    return count if len(chips) % count == 0 and count <= 2 else 1


def solution(mesh):
    Y = inner_count(mesh)
    Z = mesh.shape["tp"] // Y
    in_specs = (
        P("rep", ("tp", "sub")),
        P(("tp", "sub"), None),
        P("rep", ("tp", "sub")),
        P(("tp", "sub")),
    )
    out_specs = (P("rep", None), P("rep", None), P("rep", ("tp", "sub")))
    return jax.shard_map(
        functools.partial(per_device, Y, Z, mesh.shape["sub"]),
        mesh=mesh, in_specs=in_specs, out_specs=out_specs, check_vma=False,
    )
```

```python
import functools

import jax
import jax.numpy as jnp
from jax import lax
from jax.experimental import pallas as pl
from jax.experimental.pallas import tpu as pltpu
from jax.sharding import PartitionSpec as P

BLOCK = 128
LANES = 128
ROWS_STEP = 128
GRANT = 40 * 1024 * 1024
MESH = pl.DeviceIdType.MESH

epsilon = 0.1
floor_scale = 0.5


def loop(n, body):
    if n <= 8:
        for i in range(n):
            body(i)
    else:
        lax.fori_loop(0, n, lambda i, c: (body(i), c)[1], 0)


def kernel(
    Y, Z, U, C, R, width_all,
    att, weight, res, gain,
    quant, stat, new_res,
    att_p, w_own, w_par, ysend, ybuf, zsend, zbuf, hid,
    l_sem, xs_sem, xr_sem, as_sem, ar_sem, ys_sem, yr_sem, zs_sem, zr_sem,
    ss_sem, sr_sem, qzs, qzr, qys, qyr, qus, qur,
):
    T = Y * Z
    n = T * U
    w = res.shape[1]
    nb = w // BLOCK
    tp = lax.axis_index("tp")
    s = lax.axis_index("sub")
    z = tp // Y
    y = lax.rem(tp, Y)
    me = tp * U + s
    other = (U - 1) - s
    f32 = jnp.float32

    def cols(t, sub):
        return pl.ds(pl.multiple_of((t * U + sub) * w, w), w)

    def rows(c):
        return pl.ds(c * R, R)

    F = LANES // R

    def sub_rows(c):
        return pl.ds((c % F) * R, R)

    def rc(src, dst, ss, rs, t, sub):
        return pltpu.make_async_remote_copy(
            src_ref=src, dst_ref=dst, send_sem=ss, recv_sem=rs,
            device_id={"tp": t, "sub": sub}, device_id_type=MESH,
        )

    yp = (Y - 1) - y
    zt = lambda zz: zz * Y + y
    zo = lambda k: lax.rem(z + k, Z)
    order = lambda i: (i % Z) * Y + (yp if i < Z else y) if Y > 1 else i

    def wload(t):
        return pltpu.make_async_copy(weight.at[:, cols(t, s)], w_own.at[t], l_sem.at[t])

    def wpush(t):
        return rc(weight.at[:, cols(t, other)], w_par.at[t], xs_sem.at[t], xr_sem.at[t], tp, other)

    apush = rc(att, att_p, as_sem, ar_sem, tp, other)

    loop(T, lambda i: wload(order(i)).start())
    barrier = pltpu.get_barrier_semaphore()

    def greet(k):
        p = lax.rem(me + k + 1, n)
        pl.semaphore_signal(
            barrier, inc=1, device_id={"tp": p // U, "sub": lax.rem(p, U)}, device_id_type=MESH
        )

    loop(n - 1, greet)
    pl.semaphore_wait(barrier, n - 1)
    apush.start()
    loop(T, lambda i: wpush(order(i)).start())
    apush.wait()

    def w_wait(t):
        wload(t).wait()
        wpush(t).wait_recv()

    def product(c, t):
        a = jnp.dot(att[rows(c), :], w_own[t], preferred_element_type=f32)
        return a + jnp.dot(att_p[rows(c), :], w_par[t], preferred_element_type=f32)

    def ycopy(c):
        return rc(ysend.at[c], ybuf.at[c], ys_sem.at[c], yr_sem.at[c], z * Y + yp, s)

    def zcopy(c, zz):
        return rc(zsend.at[c, zz], zbuf.at[c, z], zs_sem.at[c, zz], zr_sem.at[c, z], zt(zz), s)

    def zwait(c, zz):
        rc(zsend.at[c, zz], zbuf.at[c, zz], zs_sem.at[c, zz], zr_sem.at[c, zz], zt(zz), s).wait_recv()

    if Y > 1:
        for c in range(C):
            def one(zz, c=c):
                t = zz * Y + yp
                if c == 0:
                    w_wait(t)
                ysend[c, zz] = product(c, t).astype(ysend.dtype)
            loop(Z, one)
            ycopy(c).start()

    def s4(c):
        if Y > 1:
            ycopy(c).wait_recv()

        def total(zz):
            t = zt(zz)
            if c == 0:
                w_wait(t)
            a = product(c, t)
            if Y > 1:
                a = a + ybuf[c, zz].astype(f32)
            return a

        def one(k):
            zz = zo(k + 1)
            zsend[c, zz] = total(zz).astype(zsend.dtype)
            zcopy(c, zz).start()

        loop(Z - 1, one)
        hid[c // F, sub_rows(c), :] = total(z) + res[rows(c), :].astype(f32)

    def peer(k):
        p = lax.rem(me + k + 1, n)
        return p, p // U, lax.rem(p, U)

    def scopy(g, p, t, u, slot):
        return rc(stat.at[g, me], stat.at[g, slot], ss_sem.at[g, p], sr_sem.at[g, slot], t, u)

    def qz(c, zz, right):
        sl = quant.at[rows(c), cols(zt(zz), s)]
        to = jnp.minimum(z + 1, Z - 1) if right else jnp.maximum(z - 1, 0)
        d = 1 if right else 0
        return rc(sl, sl, qzs.at[c, zz, d], qzr.at[c, zz], zt(to), s)

    def qy(c, zz, yy):
        sl = quant.at[rows(c), cols(zz * Y + yy, s)]
        return rc(sl, sl, qys.at[c, zz], qyr.at[c, zz], z * Y + yp, s)

    def qu(c, t, u):
        sl = quant.at[rows(c), cols(t, u)]
        return rc(sl, sl, qus.at[c, t], qur.at[c, t], tp, other)

    can_right, can_left = z < Z - 1, z > 0

    def s5(c):
        h = hid[c // F, sub_rows(c), :]
        for k in range(Z - 1) if Z <= 8 else ():
            zz = zo(k + 1)
            zwait(c, zz)
            h = h + zbuf[c, zz].astype(f32)
        if Z > 8:
            def add(k, h):
                zz = zo(k + 1)
                zwait(c, zz)
                return h + zbuf[c, zz].astype(f32)

            h = lax.fori_loop(0, Z - 1, add, h)
        hid[c // F, sub_rows(c), :] = h
        new_res[rows(c), :] = h.astype(new_res.dtype)
        quant[rows(c), cols(tp, s)] = (h * gain[...].astype(f32)).astype(quant.dtype)
        pl.when(can_right)(lambda: qz(c, z, True).start())
        pl.when(can_left)(lambda: qz(c, z, False).start())
        if Y > 1:
            qy(c, z, y).start()
        qu(c, tp, s).start()
        if c % F == F - 1:
            g = c // F
            h = hid[g]
            sq = jnp.sum(h * h, axis=1, keepdims=True)
            stat[g, me, 0:1, :] = jnp.broadcast_to(sq, (LANES, LANES)).T[0:1, :]
            for j in range(nb):
                sl = slice(j * BLOCK, (j + 1) * BLOCK)
                top = jnp.max(jnp.abs(h[:, sl] * gain[:, sl].astype(f32)), axis=1, keepdims=True)
                stat[g, me, j + 1 : j + 2, :] = jnp.broadcast_to(top, (LANES, LANES)).T[0:1, :]

            def send(k):
                p, t, u = peer(k)
                scopy(g, p, t, u, me).start()

            loop(n - 1, send)

    def s7(c):
        def one(k):
            lo, hi = z - (k + 1), z + (k + 1)

            @pl.when(lo >= 0)
            def _():
                qz(c, lo, True).wait_recv()
                pl.when(can_right)(lambda: qz(c, lo, True).start())
                if Y > 1:
                    qy(c, lo, y).start()
                qu(c, zt(lo), s).start()

            @pl.when(hi < Z)
            def _():
                qz(c, hi, False).wait_recv()
                pl.when(can_left)(lambda: qz(c, hi, False).start())
                if Y > 1:
                    qy(c, hi, y).start()
                qu(c, zt(hi), s).start()

        loop(Z - 1, one)

    def s8(c):
        if Y > 1:
            def one(k):
                zz = zo(k)
                qy(c, zz, yp).wait_recv()
                qu(c, zz * Y + yp, s).start()

            loop(Z, one)

    def s9(c):
        loop(T, lambda t: qu(c, t, other).wait_recv())
        if c % F == F - 1:
            def w_stat(k):
                p, t, u = peer(k)
                scopy(c // F, p, t, u, p).wait_recv()

            loop(n - 1, w_stat)

    stages = (s4, s5, s7, s8, s9)
    for i in range(C + len(stages) - 1):
        for j, stage in enumerate(stages):
            if 0 <= i - j < C:
                stage(i - j)

    loop(T, lambda t: wpush(t).wait_send())
    for c in range(C):
        if Y > 1:
            ycopy(c).wait_send()
            loop(Z, lambda zz, c=c: qy(c, zz, y).wait_send())
        loop(Z - 1, lambda k, c=c: zcopy(c, zo(k + 1)).wait_send())

        def zdone(zz, c=c):
            pl.when(can_right & (zz <= z))(lambda: qz(c, zz, True).wait_send())
            pl.when(can_left & (zz >= z))(lambda: qz(c, zz, False).wait_send())

        loop(Z, zdone)
        loop(T, lambda t, c=c: qu(c, t, s).wait_send())
        if c % F == F - 1:
            def pdone(k, c=c):
                p, t, u = peer(k)
                scopy(c // F, p, t, u, me).wait_send()

            loop(n - 1, pdone)


def finish(width_all, nb, hb, stat, res_in, quant, scales_t, res_out, full):
    n = stat.shape[1]
    total = jnp.sum(stat[0, :, 0:1, :], axis=0)
    inv = lax.rsqrt(total / width_all + epsilon)
    for d in range(n):
        full[d * nb : (d + 1) * nb, :] = stat[0, d, 1:, :]
    sc = jnp.maximum(full[...] * inv, floor_scale).astype(jnp.bfloat16)
    scales_t[...] = sc[: n * nb, :]
    factor = (inv / sc.astype(jnp.float32)).T
    for j in range(n * nb):
        sl = slice(j * BLOCK, (j + 1) * BLOCK)
        quant[:, sl] = (hb[:, sl].astype(jnp.float32) * factor[:, j : j + 1]).astype(quant.dtype)
    res_out[...] = res_in[...]


def per_device(Y, Z, U, attention, out_weight, residual, norm_gain):
    M, K = attention.shape
    width_all = out_weight.shape[1]
    w = residual.shape[1]
    T = Y * Z
    n = T * U
    R = ROWS_STEP
    C = M // R
    G = M // LANES
    nb = w // BLOCK
    bf = jnp.bfloat16
    f32 = jnp.float32
    dma = pltpu.SemaphoreType.DMA
    vm = pl.BlockSpec(memory_space=pltpu.VMEM)
    hb, stat, kept = pl.pallas_call(
        functools.partial(kernel, Y, Z, U, C, R, width_all),
        out_shape=(
            pltpu.VMEM((M, width_all), bf),
            pltpu.VMEM((G, n, 1 + nb, LANES), f32),
            pltpu.VMEM((M, w), bf),
        ),
        in_specs=[vm, pl.BlockSpec(memory_space=pl.ANY), vm, vm],
        out_specs=(vm, vm, vm),
        scratch_shapes=[
            pltpu.VMEM((M, K), bf),
            pltpu.VMEM((T, K, w), bf),
            pltpu.VMEM((T, K, w), bf),
            pltpu.VMEM((C, Z, R, w), bf),
            pltpu.VMEM((C, Z, R, w), bf),
            pltpu.VMEM((C, Z, R, w), bf),
            pltpu.VMEM((C, Z, R, w), bf),
            pltpu.VMEM((G, LANES, w), f32),
            dma((T,)), dma((T,)), dma((T,)), dma, dma,
            dma((C,)), dma((C,)), dma((C, Z)), dma((C, Z)),
            dma((G, n)), dma((G, n)),
            dma((C, Z, 2)), dma((C, Z)), dma((C, Z)), dma((C, Z)), dma((C, T)), dma((C, T)),
        ],
        compiler_params=pltpu.CompilerParams(
            collective_id=0, has_side_effects=True, vmem_limit_bytes=GRANT
        ),
        cost_estimate=pl.CostEstimate(
            flops=2 * M * K * width_all, bytes_accessed=2 * K * width_all, transcendentals=0
        ),
    )(attention, out_weight, residual, norm_gain.reshape(1, w))
    quant, scales_t, new_res = pl.pallas_call(
        functools.partial(finish, width_all, nb),
        grid=(G,),
        out_shape=(
            jax.ShapeDtypeStruct((M, width_all), bf),
            jax.ShapeDtypeStruct((n * nb, M), bf),
            jax.ShapeDtypeStruct((M, w), bf),
        ),
        in_specs=[
            pl.BlockSpec((LANES, width_all), lambda i: (i, 0)),
            pl.BlockSpec((1, n, 1 + nb, LANES), lambda i: (i, 0, 0, 0)),
            pl.BlockSpec((LANES, w), lambda i: (i, 0)),
        ],
        out_specs=(
            pl.BlockSpec((LANES, width_all), lambda i: (i, 0)),
            pl.BlockSpec((n * nb, LANES), lambda i: (0, i)),
            pl.BlockSpec((LANES, w), lambda i: (i, 0)),
        ),
        scratch_shapes=[pltpu.VMEM((-(-n * nb // LANES) * LANES, LANES), f32)],
        compiler_params=pltpu.CompilerParams(vmem_limit_bytes=24 * 1024 * 1024),
    )(hb, stat, kept)
    return quant, scales_t.T, new_res


def inner_count(mesh):
    chips = [tuple(getattr(d, "coords", (0, 0, i))) for i, d in enumerate(mesh.devices[0, :, 0].flat)]
    count = sum(1 for c in chips if c[2] == chips[0][2])
    return count if len(chips) % count == 0 and count <= 2 else 1


def solution(mesh):
    Y = inner_count(mesh)
    Z = mesh.shape["tp"] // Y
    in_specs = (
        P("rep", ("tp", "sub")),
        P(("tp", "sub"), None),
        P("rep", ("tp", "sub")),
        P(("tp", "sub")),
    )
    out_specs = (P("rep", None), P("rep", None), P("rep", ("tp", "sub")))
    return jax.shard_map(
        functools.partial(per_device, Y, Z, mesh.shape["sub"]),
        mesh=mesh, in_specs=in_specs, out_specs=out_specs, check_vma=False,
    )
```

```python
import functools

import jax
import jax.numpy as jnp
from jax import lax
from jax.experimental import pallas as pl
from jax.experimental.pallas import tpu as pltpu
from jax.sharding import PartitionSpec as P

BLOCK = 128
LANES = 128
ROWS_STEP = 128
EARLY = 0
LAG = 2
GRANT = 40 * 1024 * 1024
MESH = pl.DeviceIdType.MESH

epsilon = 0.1
floor_scale = 0.5


def loop(n, body):
    if n <= 8:
        for i in range(n):
            body(i)
    else:
        lax.fori_loop(0, n, lambda i, c: (body(i), c)[1], 0)


def kernel(
    Y, Z, U, C, R, width_all,
    att_in, weight, res_in, gain,
    quant, stat, new_res,
    att_p, w_own, w_par, ysend, ybuf, zsend, zbuf, hid,
    l_sem, xs_sem, xr_sem, as_sem, ar_sem, ys_sem, yr_sem, zs_sem, zr_sem,
    ss_sem, sr_sem, qzs, qzr, qys, qyr, qus, qur, att, res, al_sem, rl_sem,
):
    T = Y * Z
    n = T * U
    w = res_in.shape[1]
    nb = w // BLOCK
    tp = lax.axis_index("tp")
    s = lax.axis_index("sub")
    z = tp // Y
    y = lax.rem(tp, Y)
    me = tp * U + s
    other = (U - 1) - s
    f32 = jnp.float32

    def cols(t, sub):
        return pl.ds(pl.multiple_of((t * U + sub) * w, w), w)

    def rows(c):
        return pl.ds(c * R, R)

    F = LANES // R

    def sub_rows(c):
        return pl.ds((c % F) * R, R)

    def rc(src, dst, ss, rs, t, sub):
        return pltpu.make_async_remote_copy(
            src_ref=src, dst_ref=dst, send_sem=ss, recv_sem=rs,
            device_id={"tp": t, "sub": sub}, device_id_type=MESH,
        )

    yp = (Y - 1) - y
    zt = lambda zz: zz * Y + y
    zo = lambda k: lax.rem(z + k, Z)
    order = lambda i: (i % Z) * Y + (yp if i < Z else y) if Y > 1 else i

    def wload(t):
        return pltpu.make_async_copy(weight.at[:, cols(t, s)], w_own.at[t], l_sem.at[t])

    def wpush(t):
        return rc(weight.at[:, cols(t, other)], w_par.at[t], xs_sem.at[t], xr_sem.at[t], tp, other)

    aload = pltpu.make_async_copy(att_in, att, al_sem)
    rload = pltpu.make_async_copy(res_in, res, rl_sem)
    apush = rc(att_in, att_p, as_sem, ar_sem, tp, other)

    aload.start()
    loop(T, lambda i: wload(order(i)).start())
    rload.start()
    barrier = pltpu.get_barrier_semaphore()

    def greet(k):
        p = lax.rem(me + k + 1, n)
        pl.semaphore_signal(
            barrier, inc=1, device_id={"tp": p // U, "sub": lax.rem(p, U)}, device_id_type=MESH
        )

    loop(n - 1, greet)
    pl.semaphore_wait(barrier, n - 1)
    apush.start()
    loop(T, lambda i: wpush(order(i)).start())
    aload.wait()
    apush.wait()
    rload.wait()

    def w_wait(t):
        wload(t).wait()
        wpush(t).wait_recv()

    def product(c, t):
        a = jnp.dot(att[rows(c), :], w_own[t], preferred_element_type=f32)
        return a + jnp.dot(att_p[rows(c), :], w_par[t], preferred_element_type=f32)

    def ycopy(c):
        return rc(ysend.at[c], ybuf.at[c], ys_sem.at[c], yr_sem.at[c], z * Y + yp, s)

    def zcopy(c, zz):
        return rc(zsend.at[c, zz], zbuf.at[c, z], zs_sem.at[c, zz], zr_sem.at[c, z], zt(zz), s)

    def zwait(c, zz):
        rc(zsend.at[c, zz], zbuf.at[c, zz], zs_sem.at[c, zz], zr_sem.at[c, zz], zt(zz), s).wait_recv()

    if Y > 1:
        for c in range(C):
            def one(zz, c=c):
                t = zz * Y + yp
                if c == 0:
                    w_wait(t)
                ysend[c, zz] = product(c, t).astype(ysend.dtype)
            loop(Z, one)
            ycopy(c).start()

    def s4(c):
        if Y > 1:
            ycopy(c).wait_recv()

        def total(zz):
            t = zt(zz)
            if c == 0:
                w_wait(t)
            a = product(c, t)
            if Y > 1:
                a = a + ybuf[c, zz].astype(f32)
            return a

        def one(k):
            zz = zo(k + 1)
            zsend[c, zz] = total(zz).astype(zsend.dtype)
            zcopy(c, zz).start()

        loop(Z - 1, one)
        hid[c // F, sub_rows(c), :] = total(z) + res[rows(c), :].astype(f32)

    def peer(k):
        p = lax.rem(me + k + 1, n)
        return p, p // U, lax.rem(p, U)

    def scopy(g, p, t, u, slot):
        return rc(stat.at[g, me], stat.at[g, slot], ss_sem.at[g, p], sr_sem.at[g, slot], t, u)

    def early(c):
        return Y > 1 and c >= C - EARLY

    def qz(c, zz, right, b=0):
        sl = quant.at[rows(c), cols(zz * Y + (yp if b else y), s)]
        to = jnp.minimum(z + 1, Z - 1) if right else jnp.maximum(z - 1, 0)
        d = 1 if right else 0
        return rc(sl, sl, qzs.at[c, zz, d, b], qzr.at[c, zz, b], zt(to), s)

    def qy(c, zz, yy):
        sl = quant.at[rows(c), cols(zz * Y + yy, s)]
        return rc(sl, sl, qys.at[c, zz], qyr.at[c, zz], z * Y + yp, s)

    def qu(c, t, u):
        sl = quant.at[rows(c), cols(t, u)]
        return rc(sl, sl, qus.at[c, t], qur.at[c, t], tp, other)

    can_right, can_left = z < Z - 1, z > 0

    def s5(c):
        h = hid[c // F, sub_rows(c), :]
        for k in range(Z - 1) if Z <= 8 else ():
            zz = zo(k + 1)
            zwait(c, zz)
            h = h + zbuf[c, zz].astype(f32)
        if Z > 8:
            def add(k, h):
                zz = zo(k + 1)
                zwait(c, zz)
                return h + zbuf[c, zz].astype(f32)

            h = lax.fori_loop(0, Z - 1, add, h)
        hid[c // F, sub_rows(c), :] = h
        new_res[rows(c), :] = h.astype(new_res.dtype)
        quant[rows(c), cols(tp, s)] = (h * gain[...].astype(f32)).astype(quant.dtype)
        pl.when(can_right)(lambda: qz(c, z, True).start())
        pl.when(can_left)(lambda: qz(c, z, False).start())
        if Y > 1:
            qy(c, z, y).start()
        qu(c, tp, s).start()
        if c % F == F - 1:
            g = c // F
            h = hid[g]
            sq = jnp.sum(h * h, axis=1, keepdims=True)
            stat[g, me, 0:1, :] = jnp.broadcast_to(sq, (LANES, LANES)).T[0:1, :]
            for j in range(nb):
                sl = slice(j * BLOCK, (j + 1) * BLOCK)
                top = jnp.max(jnp.abs(h[:, sl] * gain[:, sl].astype(f32)), axis=1, keepdims=True)
                stat[g, me, j + 1 : j + 2, :] = jnp.broadcast_to(top, (LANES, LANES)).T[0:1, :]

            def send(k):
                p, t, u = peer(k)
                scopy(g, p, t, u, me).start()

            loop(n - 1, send)

    def s7(c):
        def hop(zz, right, b):
            qz(c, zz, right, b).wait_recv()
            pl.when(can_right if right else can_left)(lambda: qz(c, zz, right, b).start())
            if Y > 1 and not early(c):
                qy(c, zz, y).start()
            qu(c, zz * Y + (yp if b else y), s).start()

        if early(c):
            qy(c, z, yp).wait_recv()
            pl.when(can_right)(lambda: qz(c, z, True, 1).start())
            pl.when(can_left)(lambda: qz(c, z, False, 1).start())
            qu(c, z * Y + yp, s).start()

        def one(k):
            for b in (0, 1) if early(c) else (0,):
                lo, hi = z - (k + 1), z + (k + 1)
                pl.when(lo >= 0)(lambda: hop(lo, True, b))
                pl.when(hi < Z)(lambda: hop(hi, False, b))

        loop(Z - 1, one)

    def s8(c):
        if Y > 1 and not early(c):
            def one(k):
                zz = zo(k)
                qy(c, zz, yp).wait_recv()
                qu(c, zz * Y + yp, s).start()

            loop(Z, one)

    def s9(c):
        loop(T, lambda t: qu(c, t, other).wait_recv())
        if c % F == F - 1:
            def w_stat(k):
                p, t, u = peer(k)
                scopy(c // F, p, t, u, p).wait_recv()

            loop(n - 1, w_stat)

    stages = ((0, s4), (1, s5), (LAG, s7), (LAG + 1, s8), (C + LAG + 1, s9))
    for i in range(2 * C + LAG + 1):
        for lag, stage in stages:
            if 0 <= i - lag < C:
                stage(i - lag)

    loop(T, lambda t: wpush(t).wait_send())
    for c in range(C):
        if Y > 1:
            ycopy(c).wait_send()
            if early(c):
                qy(c, z, y).wait_send()
            else:
                loop(Z, lambda zz, c=c: qy(c, zz, y).wait_send())
        loop(Z - 1, lambda k, c=c: zcopy(c, zo(k + 1)).wait_send())

        def zdone(zz, c=c):
            for b in (0, 1) if early(c) else (0,):
                pl.when(can_right & (zz <= z))(lambda: qz(c, zz, True, b).wait_send())
                pl.when(can_left & (zz >= z))(lambda: qz(c, zz, False, b).wait_send())

        loop(Z, zdone)
        loop(T, lambda t, c=c: qu(c, t, s).wait_send())
        if c % F == F - 1:
            def pdone(k, c=c):
                p, t, u = peer(k)
                scopy(c // F, p, t, u, me).wait_send()

            loop(n - 1, pdone)


def finish(width_all, nb, hb, stat, res_in, quant, scales_t, res_out, full):
    n = stat.shape[1]
    total = jnp.sum(stat[0, :, 0:1, :], axis=0)
    inv = lax.rsqrt(total / width_all + epsilon)
    for d in range(n):
        full[d * nb : (d + 1) * nb, :] = stat[0, d, 1:, :]
    sc = jnp.maximum(full[...] * inv, floor_scale).astype(jnp.bfloat16)
    scales_t[...] = sc[: n * nb, :]
    factor = (inv / sc.astype(jnp.float32)).T
    for j in range(n * nb):
        sl = slice(j * BLOCK, (j + 1) * BLOCK)
        quant[:, sl] = (hb[:, sl].astype(jnp.float32) * factor[:, j : j + 1]).astype(quant.dtype)
    res_out[...] = res_in[...]


def per_device(Y, Z, U, attention, out_weight, residual, norm_gain):
    M, K = attention.shape
    width_all = out_weight.shape[1]
    w = residual.shape[1]
    T = Y * Z
    n = T * U
    R = ROWS_STEP
    C = M // R
    G = M // LANES
    nb = w // BLOCK
    bf = jnp.bfloat16
    f32 = jnp.float32
    dma = pltpu.SemaphoreType.DMA
    vm = pl.BlockSpec(memory_space=pltpu.VMEM)
    hbm = pl.BlockSpec(memory_space=pltpu.HBM)
    hb, stat, kept = pl.pallas_call(
        functools.partial(kernel, Y, Z, U, C, R, width_all),
        out_shape=(
            pltpu.VMEM((M, width_all), bf),
            pltpu.VMEM((G, n, 1 + nb, LANES), f32),
            pltpu.VMEM((M, w), bf),
        ),
        in_specs=[hbm, hbm, hbm, vm],
        out_specs=(vm, vm, vm),
        scratch_shapes=[
            pltpu.VMEM((M, K), bf),
            pltpu.VMEM((T, K, w), bf),
            pltpu.VMEM((T, K, w), bf),
            pltpu.VMEM((C, Z, R, w), bf),
            pltpu.VMEM((C, Z, R, w), bf),
            pltpu.VMEM((C, Z, R, w), bf),
            pltpu.VMEM((C, Z, R, w), bf),
            pltpu.VMEM((G, LANES, w), f32),
            dma((T,)), dma((T,)), dma((T,)), dma, dma,
            dma((C,)), dma((C,)), dma((C, Z)), dma((C, Z)),
            dma((G, n)), dma((G, n)),
            dma((C, Z, 2, 2)), dma((C, Z, 2)), dma((C, Z)), dma((C, Z)), dma((C, T)), dma((C, T)),
            pltpu.VMEM((M, K), bf), pltpu.VMEM((M, w), bf), dma, dma,
        ],
        compiler_params=pltpu.CompilerParams(
            collective_id=0, has_side_effects=True, vmem_limit_bytes=GRANT
        ),
        cost_estimate=pl.CostEstimate(
            flops=2 * M * K * width_all, bytes_accessed=2 * K * width_all, transcendentals=0
        ),
    )(attention, out_weight, residual, norm_gain.reshape(1, w))
    quant, scales_t, new_res = pl.pallas_call(
        functools.partial(finish, width_all, nb),
        grid=(G,),
        out_shape=(
            jax.ShapeDtypeStruct((M, width_all), bf),
            jax.ShapeDtypeStruct((n * nb, M), bf),
            jax.ShapeDtypeStruct((M, w), bf),
        ),
        in_specs=[
            pl.BlockSpec((LANES, width_all), lambda i: (i, 0)),
            pl.BlockSpec((1, n, 1 + nb, LANES), lambda i: (i, 0, 0, 0)),
            pl.BlockSpec((LANES, w), lambda i: (i, 0)),
        ],
        out_specs=(
            pl.BlockSpec((LANES, width_all), lambda i: (i, 0)),
            pl.BlockSpec((n * nb, LANES), lambda i: (0, i)),
            pl.BlockSpec((LANES, w), lambda i: (i, 0)),
        ),
        scratch_shapes=[pltpu.VMEM((-(-n * nb // LANES) * LANES, LANES), f32)],
        compiler_params=pltpu.CompilerParams(vmem_limit_bytes=24 * 1024 * 1024),
    )(hb, stat, kept)
    return quant, scales_t.T, new_res


def inner_count(mesh):
    chips = [tuple(getattr(d, "coords", (0, 0, i))) for i, d in enumerate(mesh.devices[0, :, 0].flat)]
    count = sum(1 for c in chips if c[2] == chips[0][2])
    return count if len(chips) % count == 0 and count <= 2 else 1


def solution(mesh):
    Y = inner_count(mesh)
    Z = mesh.shape["tp"] // Y
    in_specs = (
        P("rep", ("tp", "sub")),
        P(("tp", "sub"), None),
        P("rep", ("tp", "sub")),
        P(("tp", "sub")),
    )
    out_specs = (P("rep", None), P("rep", None), P("rep", ("tp", "sub")))
    return jax.shard_map(
        functools.partial(per_device, Y, Z, mesh.shape["sub"]),
        mesh=mesh, in_specs=in_specs, out_specs=out_specs, check_vma=False,
    )
```
